32 devices in a mesh: gx: 4 (over y, x), gy: 4 (over z), gz: 2 (over core).
Axes of the slice: x: 2, y: 2, z: 4, core: 2. Of those that a mesh axis runs over, the one named last changes fastest.
Arguments:
- right_side: float32 [128, 128, 256], P('gx', 'gy', 'gz'), may hold values from -1 to 1
- z_faces: float32 [256], P('gz'), may hold values from 0.5 to 2, as said below
- xy_coupling: float32 [5], replicated, as said below
- block_inverse: float32 [5, 256, 128], P(None, 'gz'), as said below
Outputs:
- solution: float32 [128, 128, 256], P('gx', 'gy', 'gz')
- residual: float32 [128, 128, 256], P('gx', 'gy', 'gz')
The draws below stay inside these ranges and needn't reach their ends.
Inputs may be any that keep to these rules, and one draw needn't show every extreme that they name: z_faces is positive. xy_coupling[l] lies between 2.9 * 4^-l / 128^2 and 5.5 * 4^-l / 128^2. block_inverse[l] holds, block by block, the inverses of the 128 x 128 diagonal blocks of M_l built from z_faces and xy_coupling[l].
All inputs are finite; a program needn't handle non-finite values.
Results may differ from the reference program's by a relative error of at most 0.028.
Values sent between devices are 32-bit elements; how exact they have to be, the bound alone decides.
A program may use at most 128 MiB of HBM per device.

```python
import jax
import jax.numpy as jnp
from jax import lax

CZ = 128
LEVELS = 5
SWEEPS = 2
NX = 128
NY = 128
NZ = 256


def coefficient_set(key):
    face_key = jax.random.fold_in(key, 101)
    level_key = jax.random.fold_in(key, 202)
    face_values = jnp.exp(jax.random.uniform(face_key, (NZ,), jnp.float32, jnp.log(0.5), jnp.log(2.0)))
    spread = jnp.exp(jax.random.uniform(level_key, (LEVELS,), jnp.float32, -0.3, 0.3))
    lateral = 4.0 / (CZ * CZ) * spread * 0.25 ** jnp.arange(LEVELS).astype(jnp.float32)
    return (face_values, lateral)


def draw_right_side(key, part):
    rough_key = jax.random.fold_in(key, 303)
    amplitude = 0.03
    rough = jnp.clip(jax.random.normal(rough_key, (NX, NY, NZ), jnp.float32), -4.0, 4.0)
    field = amplitude * rough
    return field.astype(jnp.float32)


def draw_z_faces(key, part):
    return coefficient_set(key)[0].astype(jnp.float32)


def draw_xy_coupling(key, part):
    return coefficient_set(key)[1].astype(jnp.float32)


def draw_block_inverse(key, part):
    face_values, lateral = coefficient_set(key)
    blocks_count = NZ // CZ
    up_values = jnp.concatenate([face_values[1:], jnp.ones((1,), jnp.float32)])
    down_rows = face_values.reshape(blocks_count, CZ)
    up_rows = up_values.reshape(blocks_count, CZ)
    identity = jnp.eye(CZ, dtype=jnp.float32)
    upper_shift = jnp.eye(CZ, k=1, dtype=jnp.float32)
    coupling = up_rows[:, :, None] * upper_shift
    base_matrix = (down_rows + up_rows)[:, :, None] * identity - coupling - jnp.swapaxes(coupling, 1, 2)
    matrices = base_matrix[None] + (4.0 * lateral)[:, None, None, None] * identity
    return jnp.linalg.inv(matrices).reshape(LEVELS, NZ, CZ).astype(jnp.float32)


def setup_inputs(seed: int = 0) -> dict:
    streams_of = jax.random.split(jax.random.key(seed), 5)
    right_side = draw_right_side(jax.random.fold_in(streams_of[4], 71), 0)
    z_faces = draw_z_faces(jax.random.fold_in(streams_of[4], 71), 0)
    xy_coupling = draw_xy_coupling(jax.random.fold_in(streams_of[4], 71), 0)
    block_inverse = draw_block_inverse(jax.random.fold_in(streams_of[4], 71), 0)
    return {"right_side": right_side, "z_faces": z_faces, "xy_coupling": xy_coupling, "block_inverse": block_inverse}


damping = 0.8
highest = lax.Precision.HIGHEST

def interface_setup(corner_aa, corner_ab, corner_ba, corner_bb, couplings):
    determinant = corner_aa * corner_bb - corner_ab * corner_ba
    corner_inverse = jnp.stack([jnp.stack([corner_bb, -corner_ab], -1), jnp.stack([-corner_ba, corner_aa], -1)], -2) / determinant[:, None, None]
    blocks_count = corner_aa.shape[0]
    identity = jnp.eye(blocks_count, dtype=corner_inverse.dtype)
    diagonal_part = jnp.einsum('kab,kl->kalb', corner_inverse, identity, precision=highest).reshape(2 * blocks_count, 2 * blocks_count)
    link_values = jnp.zeros((2 * blocks_count - 1,), corner_inverse.dtype).at[1::2].set(-couplings)
    schur_matrix = diagonal_part + jnp.diag(link_values, 1) + jnp.diag(link_values, -1)
    return (corner_inverse, diagonal_part, jnp.linalg.cholesky(schur_matrix))

def level_setup(block_inverse, z_faces, level):
    block_len = block_inverse.shape[2]
    blocks_count = z_faces.shape[0] // block_len
    inverse_blocks = block_inverse[level].reshape(blocks_count, block_len, block_len)
    last_cell = block_len - 1
    couplings = z_faces.reshape(blocks_count, block_len)[1:, 0]
    corner_inverse, diagonal_part, factor = interface_setup(inverse_blocks[:, 0, 0], inverse_blocks[:, 0, last_cell], inverse_blocks[:, last_cell, 0], inverse_blocks[:, last_cell, last_cell], couplings)
    return (inverse_blocks, corner_inverse, factor, couplings)

def line_solve(source, inverse_blocks, corner_inverse, factor, couplings):
    first_extent, second_extent, depth = source.shape
    blocks_count, block_len = (inverse_blocks.shape[0], inverse_blocks.shape[1])
    blocked = source.reshape(first_extent, second_extent, blocks_count, block_len)
    local_part = jnp.einsum('xykj,kij->xyki', blocked, inverse_blocks, precision=highest)
    end_values = jnp.stack([local_part[..., 0], local_part[..., block_len - 1]], -1)
    reduced_source = jnp.einsum('kab,xykb->kaxy', corner_inverse, end_values, precision=highest).reshape(2 * blocks_count, first_extent * second_extent)
    forward = lax.linalg.triangular_solve(factor, reduced_source, left_side=True, lower=True)
    interfaces = lax.linalg.triangular_solve(factor, forward, left_side=True, lower=True, transpose_a=True)
    interfaces = interfaces.reshape(blocks_count, 2, first_extent, second_extent).transpose(2, 3, 0, 1)
    zero_plane = jnp.zeros((first_extent, second_extent, 1), local_part.dtype)
    below_last = jnp.concatenate([zero_plane, interfaces[:, :, :-1, 1]], 2)
    above_first = jnp.concatenate([interfaces[:, :, 1:, 0], zero_plane], 2)
    zero_single = jnp.zeros((1,), couplings.dtype)
    down_coupling = jnp.concatenate([zero_single, couplings])
    up_coupling = jnp.concatenate([couplings, zero_single])
    result = local_part + (down_coupling * below_last)[..., None] * inverse_blocks[:, :, 0] + (up_coupling * above_first)[..., None] * inverse_blocks[:, :, block_len - 1]
    return result.reshape(first_extent, second_extent, depth)

def apply_operator(iterate, lateral_weight, down_faces, up_faces):
    padded = jnp.pad(iterate, 1)
    lateral = padded[:-2, 1:-1, 1:-1] + padded[2:, 1:-1, 1:-1] + padded[1:-1, :-2, 1:-1] + padded[1:-1, 2:, 1:-1]
    return lateral_weight * (4.0 * iterate - lateral) + down_faces * (iterate - padded[1:-1, 1:-1, :-2]) + up_faces * (iterate - padded[1:-1, 1:-1, 2:])

def restrict(field):
    first_extent, second_extent, depth = field.shape
    return field.reshape(first_extent // 2, 2, second_extent // 2, 2, depth).sum(axis=(1, 3)) * 0.25

def prolong(padded):
    first_extent = padded.shape[0] - 2
    second_extent = padded.shape[1] - 2
    depth = padded.shape[2]
    even_rows = 0.75 * padded[1:-1] + 0.25 * padded[:-2]
    odd_rows = 0.75 * padded[1:-1] + 0.25 * padded[2:]
    widened = jnp.stack([even_rows, odd_rows], 1).reshape(2 * first_extent, second_extent + 2, depth)
    even_rows = 0.75 * widened[:, 1:-1] + 0.25 * widened[:, :-2]
    odd_rows = 0.75 * widened[:, 1:-1] + 0.25 * widened[:, 2:]
    return jnp.stack([even_rows, odd_rows], 2).reshape(2 * first_extent, 2 * second_extent, depth)

def reference(right_side, z_faces, xy_coupling, block_inverse):
    up_faces = jnp.concatenate([z_faces[1:], jnp.ones((1,), z_faces.dtype)])
    setups = [level_setup(block_inverse, z_faces, level) for level in range(LEVELS)]

    def operator(iterate, level):
        return apply_operator(iterate, xy_coupling[level], z_faces, up_faces)

    def smooth(source, level):
        return line_solve(source, *setups[level])

    def multigrid_cycle(source, level):
        iterate = damping * smooth(source, level)
        for sweep in range(SWEEPS - 1):
            iterate = iterate + damping * smooth(source - operator(iterate, level), level)
        if level == LEVELS - 1:
            return iterate
        coarse = multigrid_cycle(restrict(source - operator(iterate, level)), level + 1)
        iterate = iterate + prolong(jnp.pad(coarse, ((1, 1), (1, 1), (0, 0))))
        for sweep in range(SWEEPS):
            iterate = iterate + damping * smooth(source - operator(iterate, level), level)
        return iterate
    solution = multigrid_cycle(right_side, 0)
    return (solution, right_side - operator(solution, 0))
```

```python
import functools

import jax
import jax.numpy as jnp
from jax import lax
from jax.experimental import pallas as pl
from jax.experimental.pallas import tpu as pltpu
from jax.sharding import PartitionSpec as P

LEVELS = 5
SWEEPS = 2


damping = 0.8
highest = lax.Precision.HIGHEST


def extended(cells, sides, width):
    for axis, dim in sides:
        count = lax.axis_size(axis)
        ends = count - 1
        head = lax.slice_in_dim(cells, 0, width, axis=dim)
        tail = lax.slice_in_dim(cells, cells.shape[dim] - width, cells.shape[dim], axis=dim)
        cells = jnp.concatenate(
            [
                lax.ppermute(tail, axis, [(i, (i + 1) % count) for i in range(ends)]),
                cells,
                lax.ppermute(head, axis, [((i + 1) % count, i) for i in range(ends)]),
            ],
            axis=dim,
        )
    return cells


def interface_setup(corner_aa, corner_ab, corner_ba, corner_bb, couplings):
    determinant = corner_aa * corner_bb - corner_ab * corner_ba
    corner_inverse = (
        jnp.stack(
            [jnp.stack([corner_bb, -corner_ab], -1), jnp.stack([-corner_ba, corner_aa], -1)], -2
        )
        / determinant[:, None, None]
    )
    blocks_count = corner_aa.shape[0]
    identity = jnp.eye(blocks_count, dtype=corner_inverse.dtype)
    diagonal_part = jnp.einsum("kab,kl->kalb", corner_inverse, identity, precision=highest).reshape(
        2 * blocks_count, 2 * blocks_count
    )
    link_values = jnp.zeros((2 * blocks_count - 1,), corner_inverse.dtype).at[1::2].set(-couplings)
    schur_matrix = diagonal_part + jnp.diag(link_values, 1) + jnp.diag(link_values, -1)
    return (corner_inverse, diagonal_part, jnp.linalg.cholesky(schur_matrix))


def make_solver(inverse_block, corner_rows, couplings, device_index, down_coupling, up_coupling):
    corner_inverse, diagonal_part, factor = interface_setup(
        corner_rows[:, 0], corner_rows[:, 1], corner_rows[:, 2], corner_rows[:, 3], couplings
    )
    block_len = inverse_block.shape[0]
    forward = lax.linalg.triangular_solve(factor, diagonal_part, left_side=True, lower=True)
    reach = lax.linalg.triangular_solve(
        factor, forward, left_side=True, lower=True, transpose_a=True
    )
    padded_reach = jnp.pad(reach, ((1, 1), (0, 0)))
    slice_rows = lax.dynamic_slice_in_dim(padded_reach, 2 * device_index, 4, 0)
    needed = jnp.stack([slice_rows[0], slice_rows[3]])

    def neighbours(end_values):
        zero_carry = jnp.zeros(end_values.shape, jnp.float32)
        nearby = zero_carry + jnp.dot(
            needed, lax.all_gather(end_values, "gz", axis=0, tiled=True), precision=highest
        )
        return (nearby[0], nearby[1])

    def solve(source):
        first_extent, second_extent, depth = source.shape
        line_count = first_extent * second_extent
        local_part = jnp.einsum("xyj,ij->xyi", source, inverse_block, precision=highest)
        end_values = jnp.stack(
            [
                local_part[:, :, 0].reshape(line_count),
                local_part[:, :, block_len - 1].reshape(line_count),
            ]
        )
        below_last, above_first = neighbours(end_values)
        return (
            local_part
            + (down_coupling * below_last).reshape(first_extent, second_extent, 1)
            * inverse_block[:, 0]
            + (up_coupling * above_first).reshape(first_extent, second_extent, 1)
            * inverse_block[:, block_len - 1]
        )

    return solve


def apply_operator(iterate, lateral_weight, down_faces, up_faces):
    padded = extended(iterate, (("gx", 0), ("gy", 1), ("gz", 2)), 1)
    lateral = (
        padded[:-2, 1:-1, 1:-1]
        + padded[2:, 1:-1, 1:-1]
        + padded[1:-1, :-2, 1:-1]
        + padded[1:-1, 2:, 1:-1]
    )
    return (
        lateral_weight * (4.0 * iterate - lateral)
        + down_faces * (iterate - padded[1:-1, 1:-1, :-2])
        + up_faces * (iterate - padded[1:-1, 1:-1, 2:])
    )


def restrict(field):
    first_extent, second_extent, depth = field.shape
    return field.reshape(first_extent // 2, 2, second_extent // 2, 2, depth).sum(axis=(1, 3)) * 0.25


def prolong(padded):
    first_extent = padded.shape[0] - 2
    second_extent = padded.shape[1] - 2
    depth = padded.shape[2]
    even_rows = 0.75 * padded[1:-1] + 0.25 * padded[:-2]
    odd_rows = 0.75 * padded[1:-1] + 0.25 * padded[2:]
    widened = jnp.stack([even_rows, odd_rows], 1).reshape(
        2 * first_extent, second_extent + 2, depth
    )
    even_rows = 0.75 * widened[:, 1:-1] + 0.25 * widened[:, :-2]
    odd_rows = 0.75 * widened[:, 1:-1] + 0.25 * widened[:, 2:]
    return jnp.stack([even_rows, odd_rows], 2).reshape(2 * first_extent, 2 * second_extent, depth)


def body(right_side, z_faces, xy_coupling, block_inverse):
    device_index = lax.axis_index("gz")
    levels_count = block_inverse.shape[0]
    last_cell = block_inverse.shape[1] - 1
    corner = jnp.stack(
        [
            block_inverse[:, 0, 0],
            block_inverse[:, 0, last_cell],
            block_inverse[:, last_cell, 0],
            block_inverse[:, last_cell, last_cell],
        ],
        -1,
    )[None]
    corners, firsts = (
        lax.all_gather(corner, "gz", axis=0, tiled=True),
        lax.all_gather(z_faces[:1], "gz", axis=0, tiled=True),
    )
    couplings = firsts[1:]
    edge_faces = jnp.concatenate([firsts, jnp.ones((1,), jnp.float32)])
    top_face = lax.dynamic_slice_in_dim(edge_faces, device_index + 1, 1, 0)
    up_faces = jnp.concatenate([z_faces[1:], top_face])
    solvers = [
        make_solver(
            block_inverse[level],
            corners[:, level],
            couplings,
            device_index,
            z_faces[0],
            top_face[0],
        )
        for level in range(levels_count)
    ]

    def operator(iterate, level):
        return apply_operator(iterate, xy_coupling[level], z_faces, up_faces)

    def multigrid_cycle(source, level):
        iterate = damping * solvers[level](source)
        iterate = iterate + damping * solvers[level](source - operator(iterate, level))
        if level == LEVELS - 1:
            return iterate
        coarse = multigrid_cycle(restrict(source - operator(iterate, level)), level + 1)
        widened = extended(coarse, (("gx", 0), ("gy", 1)), 1)
        iterate = iterate + prolong(widened)
        for sweep in range(SWEEPS):
            iterate = iterate + damping * solvers[level](source - operator(iterate, level))
        return iterate

    solution = multigrid_cycle(right_side, 0)
    return (solution, right_side - operator(solution, 0))


MESH = pl.DeviceIdType.MESH
HALOS = (4, 6, 6)
YPAD = 8


def block_range(offset, own, halo, extent):
    start = offset * own - halo
    low = max(0, start)
    high = min(extent, (offset + 1) * own + halo)
    return low, high - low, low - start


def cycle_kernel(geometry, f_ref, z_ref, e_ref, g_ref, sol_ref, res_ref, *scratch):
    gx_n, gy_n, gz_n, nx, ny, depth, levels = geometry
    (sinv, g_all, z_all, gather) = scratch[:4]
    R = scratch[4 : 4 + levels]
    U = scratch[4 + levels : 4 + 2 * levels]
    W = scratch[4 + 2 * levels : 4 + 3 * levels]
    V = scratch[4 + 3 * levels : 4 + 4 * levels]
    D = scratch[4 + 4 * levels : 4 + 5 * levels]
    (own1, own2, own3, c4u, c4d, c3u, c3d, cwu, cwd) = scratch[4 + 5 * levels : 13 + 5 * levels]
    OWN = (None, own1, own2, own3)
    (g_send, g_recv, h_send, h_recv, a_send, a_recv, o_send, o_recv) = scratch[13 + 5 * levels :]

    ix, iy, iz = lax.axis_index("gx"), lax.axis_index("gy"), lax.axis_index("gz")
    bx = ix * gz_n + iz
    bx_n = gx_n * gz_n
    f32 = jnp.float32

    def owned(level):
        return nx >> level, ny >> level

    def copy(src, dst, send, recv, device):
        return pltpu.make_async_remote_copy(
            src_ref=src,
            dst_ref=dst,
            send_sem=send,
            recv_sem=recv,
            device_id=device,
            device_id_type=MESH,
        )

    def setup_copies(other):
        here = (ix, iy, lax.rem(iz + other, gz_n))
        out = []
        for level in range(levels):
            out.append(
                copy(
                    g_ref.at[level],
                    g_all.at[level, iz],
                    g_send.at[other, level],
                    g_recv.at[other, level],
                    here,
                )
            )
        out.append(
            copy(z_ref, z_all.at[iz], g_send.at[other, levels], g_recv.at[other, levels], here)
        )
        return out

    def start_copies():
        out = []
        reach = -(-HALOS[0] // nx)
        for t in range(-reach, gz_n + reach):
            xs, xn, xd = block_range(t, nx, HALOS[0], nx * gz_n)
            dgx, target = t // gz_n, t % gz_n
            for dy in (-1, 0, 1):
                ys, yn, yd = block_range(dy, ny, YPAD, ny)
                out.append((t, dgx, target, dy, (xs, xn, xd), (ys, yn, yd)))
        return out

    plan0 = start_copies()

    def copy0(entry, source_z, device):
        t, dgx, target, dy, (xs, xn, xd), (ys, yn, yd) = entry
        slot = (t + gz_n) * 3 + dy + 1
        return copy(
            f_ref.at[pl.ds(xs, xn), pl.ds(ys, yn), :],
            R[0].at[pl.ds(xd, xn), source_z, pl.ds(yd, yn), :],
            h_send.at[0, slot],
            h_recv.at[0, slot, source_z],
            device,
        )

    def inside(x, y):
        return (x >= 0) & (x < gx_n) & (y >= 0) & (y < gy_n)

    def send0(start):
        for entry in plan0:
            t, dgx, target, dy = entry[:4]
            ok = inside(ix + dgx, iy + dy)
            if dgx == 0 and dy == 0:
                ok = ok & (iz != target)

            @pl.when(ok)
            def _():
                c = copy0(entry, iz, (ix + dgx, iy + dy, target))
                c.start() if start else c.wait_send()

    def recv0():
        for entry in plan0:
            t, dgx, target, dy = entry[:4]
            for source_z in range(gz_n):
                if dgx == 0 and dy == 0 and source_z == target:
                    continue

                @pl.when((iz == target) & inside(ix - dgx, iy - dy))
                def _():
                    copy0(entry, source_z, (ix - dgx, iy - dy, source_z)).wait_recv()

    send0(True)
    for other in range(1, gz_n):
        for c in setup_copies(other):
            c.start()

    for entry in plan0:
        t, dgx, target, dy, (xs, xn, xd) = entry[:5]
        if dgx == 0 and dy == 0:

            @pl.when(iz == target)
            def _():
                def step(i, _):
                    R[0][xd + i, target, pl.ds(YPAD, ny), :] = f_ref[xs + i]
                    return 0

                lax.fori_loop(0, xn, step, 0)

    for level in range(levels):
        g_all[level, iz] = g_ref[level]
    z_all[iz] = z_ref[...]

    for level in range(3):
        planes, zb, rows, lanes = R[level].shape
        halo = HALOS[level]
        n0, n1 = owned(level)
        reach = -(-halo // n0)
        for t in range(1, reach + 1):
            low = max(0, halo - t * n0)
            high = halo - (t - 1) * n0
            plane = jnp.zeros((high - low, zb, rows, lanes), f32)

            @pl.when(bx - t < 0)
            def _():
                R[level][low:high] = plane

            low2, high2 = planes - high, planes - low

            @pl.when(bx + t >= bx_n)
            def _():
                R[level][low2:high2] = plane

        edge = jnp.zeros((zb, YPAD, lanes), f32)

        @pl.when(iy == 0)
        def _():
            lax.fori_loop(0, planes, lambda i, c: zero_rows(R[level], i, 0, edge), 0)

        @pl.when(iy == gy_n - 1)
        def _():
            lax.fori_loop(0, planes, lambda i, c: zero_rows(R[level], i, rows - YPAD, edge), 0)

    def fill(ref):
        zero = jnp.zeros(ref.shape[1:], f32)

        def step(i, _):
            ref[i] = zero
            return 0

        lax.fori_loop(0, ref.shape[0], step, 0)

    for ref in (c4u, c4d, c3u, c3d, cwu, cwd):
        fill(ref)
    for level in range(levels):
        zero = jnp.zeros(W[level].shape[1:], f32)
        W[level][0] = zero
        W[level][W[level].shape[0] - 1] = zero

    for other in range(1, gz_n):
        for c in setup_copies(other):
            c.wait()

    def assemble(level, _):
        merged = g_all[level, 0]
        for k in range(1, gz_n):
            block = g_all[level, k]
            size, cz = merged.shape[0], block.shape[0]
            face = z_all[k][:, 0:1]
            a, d = block[0:1, 0:1], merged[size - 1 : size, size - 1 : size]
            last, first = merged[size - 1 : size], block[0:1]
            scale = face / (1.0 - face * face * a * d)
            p_row = jnp.concatenate([face * a * last, first], 1) * scale
            q_row = jnp.concatenate([last, face * d * first], 1) * scale
            top = jnp.concatenate([merged, jnp.zeros((size, cz), f32)], 1)
            low = jnp.concatenate([jnp.zeros((cz, size), f32), block], 1)
            top = top + merged[:, size - 1 : size] * p_row
            low = low + block[:, 0:1] * q_row
            merged = jnp.concatenate([top, low], 0)
        sinv[level] = (damping * merged).astype(jnp.bfloat16)
        return 0

    lax.fori_loop(0, levels, assemble, 0)

    def plane_mask(level, i):
        n0 = owned(level)[0]
        x = bx * n0 - HALOS[level] + i
        return jnp.where((x >= 0) & (x < bx_n * n0), 1.0, 0.0).astype(f32)

    def row_mask(level, rows, first, stride):
        n1 = owned(level)[1]
        y = lax.broadcasted_iota(jnp.int32, (rows, depth), 0) * stride + first
        y = y + iy * n1 - YPAD
        return jnp.where((y >= 0) & (y < gy_n * n1), 1.0, 0.0).astype(f32)

    def neighbours(level, i):
        centre = W[level][i + 1]
        rows = centre.shape[1]
        before = pltpu.roll(centre, 1, 1)
        after = pltpu.roll(centre, rows - 1, 1)
        if level > 2:
            y = lax.broadcasted_iota(jnp.int32, centre.shape, 1)
            before = jnp.where(y > 0, before, 0.0)
            after = jnp.where(y < rows - 1, after, 0.0)
        return centre, W[level][i] + W[level][i + 2] + before + after

    def sweep(level, first):
        planes, zb, rows, lanes = R[level].shape
        e = e_ref[level]
        chunk = planes
        while chunk % 2 == 0 and chunk * rows > 256:
            chunk //= 2

        def solve(s, _):
            at = s * chunk
            source = [R[level][pl.ds(at, chunk), k] for k in range(zb)]
            flat = [v.reshape(chunk * rows, lanes) for v in source]
            lhs = jnp.concatenate(flat, 1).astype(jnp.bfloat16)
            out = jnp.dot(lhs, sinv[level], preferred_element_type=f32)
            for k in range(zb):
                w = out[:, k * lanes : (k + 1) * lanes].reshape(chunk, rows, lanes)
                W[level][pl.ds(at + 1, chunk), k] = w
                U[level][pl.ds(at, chunk), k] = w if first else U[level][pl.ds(at, chunk), k] + w
                if level > 0:
                    dd = damping * source[k] - (4.0 * e) * w
                    D[level][pl.ds(at, chunk), k] = (
                        dd if first else D[level][pl.ds(at, chunk), k] + dd
                    )
            return 0

        lax.fori_loop(0, planes // chunk, solve, 0)

    def update(level):
        planes, zb, rows, lanes = R[level].shape
        e = e_ref[level]
        mask_y = row_mask(level, rows, 0, 1) if level < 3 else None

        def step(i, _):
            centre, total = neighbours(level, i)
            value = (1.0 - damping) * R[level][i] + e * total
            if level < 3:
                value = value * (mask_y * plane_mask(level, i))[None]
            R[level][i] = value
            return 0

        lax.fori_loop(0, planes, step, 0, unroll=2)

    def restrict_planes(level, dst, planes, x0, y0):
        rows = dst.shape[2]

        def step(j, _):
            for k in range(gz_n):
                total = None
                for a in (0, 1):
                    for b in (0, 1):
                        part = R[level][x0 + 2 * j + a, k, pl.ds(y0 + b, rows, 2), :]
                        total = part if total is None else total + part
                dst[j, k] = total * 0.25
            return 0

        lax.fori_loop(0, planes, step, 0)

    def prolong_planes(level, src, dst, offset, x0, y0):
        planes, zb, rows, lanes = R[level].shape
        half = rows // 2
        if level < 3:
            masks = [row_mask(level, half, b, 2) for b in (0, 1)]

        def step(j, _):
            for k in range(zb):
                def load(dx, dy):
                    return src[x0 + j + dx, k, pl.ds(y0 + dy, half), :]

                for b, dy in ((0, -1), (1, 1)):
                    mixed = [0.75 * load(dx, 0) + 0.25 * load(dx, dy) for dx in (-1, 0, 1)]
                    for a, far in ((0, 0), (1, 2)):
                        value = 0.75 * mixed[1] + 0.25 * mixed[far]
                        if level < 3:
                            value = value * (masks[b] * plane_mask(level, 2 * j + a))
                        dst[offset + 2 * j + a, k, pl.ds(b, half, 2), :] = value
            return 0

        lax.fori_loop(0, planes // 2, step, 0)

    def correct(level, coarse_u, coarse_d, x0, y0):
        planes = R[level].shape[0]
        rows = R[level].shape[2]
        e = e_ref[level]
        prolong_planes(level, coarse_u, W[level], 1, x0, y0)
        prolong_planes(level, coarse_d, V[level], 0, x0, y0)
        mask_y = row_mask(level, rows, 0, 1) if level < 3 else None

        def step(i, _):
            centre, total = neighbours(level, i)
            side = V[level][i]
            value = R[level][i] - side - (4.0 * e) * centre + e * total
            if level < 3:
                value = value * (mask_y * plane_mask(level, i))[None]
            R[level][i] = value
            U[level][i] = U[level][i] + centre
            if level > 0:
                D[level][i] = D[level][i] + side
            return 0

        lax.fori_loop(0, planes, step, 0)

    def exchange(level):
        n0, n1 = owned(level)
        halo = HALOS[level]
        own = OWN[level]
        reach = -(-halo // n0)
        window = R[level]

        def local(i, _):
            window[i + halo, :, pl.ds(YPAD, n1), :] = own[i]
            return 0

        def each(act):
            slot = 0
            for t in range(-reach, reach + 1):
                xs, xn, xd = block_range(t, n0, halo, n0)
                for dy in (-1, 0, 1):
                    if t == 0 and dy == 0:
                        continue
                    ys, yn, yd = block_range(dy, n1, YPAD, n1)
                    act(t, dy, (xs, xn, xd), (ys, yn, yd), slot)
                    slot += 1

        def build(t, dy, x, y, slot):
            there = bx + t + bx_n
            return copy(
                own.at[pl.ds(x[0], x[1]), :, pl.ds(y[0], y[1]), :],
                window.at[pl.ds(x[2], x[1]), :, pl.ds(y[2], y[1]), :],
                h_send.at[level, slot],
                h_recv.at[level, slot, 0],
                (there // gz_n - gx_n, iy + dy, lax.rem(there, gz_n)),
            )

        def valid(x, y):
            return (x >= 0) & (x < bx_n) & (y >= 0) & (y < gy_n)

        def start(t, dy, x, y, slot):
            @pl.when(valid(bx + t, iy + dy))
            def _():
                build(t, dy, x, y, slot).start()

        def finish(t, dy, x, y, slot):
            @pl.when(valid(bx - t, iy - dy))
            def _():
                build(t, dy, x, y, slot).wait_recv()

        def drain(t, dy, x, y, slot):
            @pl.when(valid(bx + t, iy + dy))
            def _():
                build(t, dy, x, y, slot).wait_send()

        each(start)
        lax.fori_loop(0, n0, local, 0)
        each(finish)
        return lambda: each(drain)

    def gather_all():
        count = bx_n * gy_n
        me = bx * gy_n + iy

        def build(other, slot_x, slot_y):
            there = other // gy_n
            return copy(
                own3,
                gather.at[slot_x, slot_y],
                a_send.at[other],
                a_recv.at[slot_x * gy_n + slot_y],
                (there // gz_n, lax.rem(other, gy_n), lax.rem(there, gz_n)),
            )

        def start(s, _):
            build(lax.rem(me + s, count), bx, iy).start()
            return 0

        def finish(s, _):
            other = lax.rem(me + s, count)
            build(other, other // gy_n, lax.rem(other, gy_n)).wait_recv()
            return 0

        def drain(s, _):
            build(lax.rem(me + s, count), bx, iy).wait_send()
            return 0

        lax.fori_loop(1, count, start, 0)
        gather[bx, iy] = own3[...]
        lax.fori_loop(1, count, finish, 0)
        n0, n1 = owned(3)

        def place(b, _):
            for i in range(n0):
                for y in range(gy_n):
                    R[3][b * n0 + i, :, pl.ds(y * n1, n1), :] = gather[b, y, i]
            return 0

        lax.fori_loop(0, bx_n, place, 0)
        return lambda: lax.fori_loop(1, count, drain, 0)

    def store_padded(level, src, dst, x0):
        rows = src.shape[2]

        def step(i, _):
            dst[x0 + i, :, pl.ds(YPAD, rows), :] = src[i]
            return 0

        lax.fori_loop(0, src.shape[0], step, 0)

    recv0()
    drains = [lambda: send0(False)]
    for level in range(3):
        sweep(level, True)
        update(level)
        sweep(level, False)
        update(level)
        n0 = owned(level + 1)[0]
        restrict_planes(level, OWN[level + 1], n0, HALOS[level], YPAD)
        drains.append(exchange(level + 1) if level < 2 else gather_all())
    sweep(3, True)
    update(3)
    sweep(3, False)
    update(3)
    restrict_planes(3, R[4], R[4].shape[0], 0, 0)
    sweep(4, True)
    update(4)
    sweep(4, False)
    store_padded(4, U[4], c4u, 1)
    store_padded(4, D[4], c4d, 1)
    correct(3, c4u, c4d, 1, YPAD)
    sweep(3, False)
    update(3)
    sweep(3, False)
    pad3 = HALOS[2] // 2 + 1
    store_padded(3, U[3], c3u, pad3)
    store_padded(3, D[3], c3d, pad3)
    n0, n1 = owned(3)
    margin = YPAD // 2
    for y in range(gy_n):

        @pl.when(iy == y)
        def _():
            def step(j, _):
                for src, dst in ((c3u, cwu), (c3d, cwd)):
                    dst[j, :, pl.ds(margin, n1 + 4 * margin), :] = src[
                        bx * n0 + j, :, pl.ds(y * n1, n1 + 4 * margin), :
                    ]
                return 0

            lax.fori_loop(0, cwu.shape[0], step, 0)

    for level in (2, 1, 0):
        if level == 2:
            correct(2, cwu, cwd, 1, YPAD)
        else:
            x0 = HALOS[level + 1] - HALOS[level] // 2
            correct(level, U[level + 1], D[level + 1], x0, YPAD // 2)
        sweep(level, False)
        update(level)
        sweep(level, False)

    def out_copies(which):
        src, dst = ((U[0], sol_ref), (R[0], res_ref))[which]
        out = []
        for other in range(1, gz_n):
            there = lax.rem(iz + other, gz_n)
            out.append(
                copy(
                    src.at[pl.ds(HALOS[0], nx), there, pl.ds(YPAD, ny), :],
                    dst.at[pl.ds(iz * nx, nx), :, :],
                    o_send.at[which, other],
                    o_recv.at[which, other],
                    (ix, iy, there),
                )
            )
        return out

    def out_local(which):
        src, dst = ((U[0], sol_ref), (R[0], res_ref))[which]

        def step(i, _):
            dst[iz * nx + i] = src[HALOS[0] + i, iz, pl.ds(YPAD, ny), :]
            return 0

        lax.fori_loop(0, nx, step, 0)

    for c in out_copies(0):
        c.start()
    update(0)
    for c in out_copies(1):
        c.start()
    out_local(0)
    out_local(1)
    for drain in drains:
        drain()
    for which in (0, 1):
        for c in out_copies(which):
            c.wait()


def zero_rows(ref, i, at, value):
    ref[i, :, pl.ds(at, YPAD), :] = value
    return 0


def fits(mesh, shape, inverse_shape):
    gx_n, gy_n, gz_n = (mesh.shape[a] for a in ("gx", "gy", "gz"))
    nx, ny = shape[0] // (gx_n * gz_n), shape[1] // gy_n
    return (
        inverse_shape[0] == LEVELS == 5
        and SWEEPS == 2
        and inverse_shape[2] == 128
        and nx % 8 == 0
        and ny % 32 == 0
        and (shape[1] >> 4) % 8 == 0
        and gz_n <= 2
    )


def fused_body(mesh, right_side, z_faces, xy_coupling, block_inverse):
    gx_n, gy_n, gz_n = (mesh.shape[a] for a in ("gx", "gy", "gz"))
    levels, _, depth = block_inverse.shape
    nx, ny = right_side.shape[0] // gz_n, right_side.shape[1]
    windows = []
    for level in range(levels):
        if level < 3:
            size = ((nx >> level) + 2 * HALOS[level], (ny >> level) + 2 * YPAD)
        else:
            size = ((nx * gx_n * gz_n) >> level, (ny * gy_n) >> level)
        windows.append((size[0], gz_n, size[1], depth))
    vmem = lambda shape: pltpu.VMEM(shape, jnp.float32)
    full3, full4 = windows[3], windows[4]
    pad3 = HALOS[2] // 2 + 1
    c4 = (full4[0] + 2, gz_n, full4[2] + 2 * YPAD, depth)
    c3 = (full3[0] + 2 * pad3, gz_n, full3[2] + 2 * YPAD, depth)
    cw = (windows[2][0] // 2 + 2, gz_n, (ny >> 3) + 20, depth)
    reach = 2 * max(-(-HALOS[k] // (nx >> k)) for k in range(3)) + 1
    slots = 3 * max(reach, 3 * gz_n + 1)
    dma = pltpu.SemaphoreType.DMA
    own = lambda k: (nx >> k, gz_n, ny >> k, depth)
    scratch = (
        [
            pltpu.VMEM((levels, gz_n * depth, gz_n * depth), jnp.bfloat16),
            vmem((levels, gz_n, depth, depth)),
            vmem((gz_n, 1, depth)),
            vmem((gx_n * gz_n, gy_n) + own(3)),
        ]
        + [vmem(w) for w in windows]
        + [vmem(w) for w in windows]
        + [vmem((w[0] + 2,) + w[1:]) for w in windows]
        + [vmem(w) for w in windows]
        + [vmem(w) for w in windows]
        + [vmem(own(1)), vmem(own(2)), vmem(own(3))]
        + [vmem(c4), vmem(c4), vmem(c3), vmem(c3), vmem(cw), vmem(cw)]
        + [dma((gz_n, levels + 1))] * 2
        + [dma((3, slots)), dma((3, slots, gz_n))]
        + [dma((gx_n * gy_n * gz_n,))] * 2
        + [dma((2, gz_n))] * 2
    )
    in_vmem = pl.BlockSpec(memory_space=pltpu.VMEM)
    return tuple(
        pl.pallas_call(
            functools.partial(cycle_kernel, (gx_n, gy_n, gz_n, nx, ny, depth, levels)),
            out_shape=[jax.ShapeDtypeStruct(right_side.shape, jnp.float32)] * 2,
            in_specs=[
                in_vmem,
                in_vmem,
                pl.BlockSpec(memory_space=pltpu.SMEM),
                in_vmem,
            ],
            out_specs=[in_vmem, in_vmem],
            scratch_shapes=scratch,
            compiler_params=pltpu.CompilerParams(
                has_side_effects=True, vmem_limit_bytes=60 * 1024 * 1024
            ),
        )(right_side, z_faces.reshape(1, -1), xy_coupling, block_inverse)
    )


def solution(mesh):
    def call(right_side, z_faces, xy_coupling, block_inverse):
        local = body
        if fits(mesh, right_side.shape, block_inverse.shape):
            local = functools.partial(fused_body, mesh)
        return jax.shard_map(
            local,
            mesh=mesh,
            in_specs=(P("gx", "gy", "gz"), P("gz"), P(), P(None, "gz", None)),
            out_specs=(P("gx", "gy", "gz"), P("gx", "gy", "gz")),
            check_vma=False,
        )(right_side, z_faces, xy_coupling, block_inverse)

    return call
```

```python
import functools

import jax
import jax.numpy as jnp
from jax import lax
from jax.experimental import pallas as pl
from jax.experimental.pallas import tpu as pltpu
from jax.sharding import PartitionSpec as P

LEVELS = 5
SWEEPS = 2


damping = 0.8
highest = lax.Precision.HIGHEST


def extended(cells, sides, width):
    for axis, dim in sides:
        count = lax.axis_size(axis)
        ends = count - 1
        head = lax.slice_in_dim(cells, 0, width, axis=dim)
        tail = lax.slice_in_dim(cells, cells.shape[dim] - width, cells.shape[dim], axis=dim)
        cells = jnp.concatenate(
            [
                lax.ppermute(tail, axis, [(i, (i + 1) % count) for i in range(ends)]),
                cells,
                lax.ppermute(head, axis, [((i + 1) % count, i) for i in range(ends)]),
            ],
            axis=dim,
        )
    return cells


def interface_setup(corner_aa, corner_ab, corner_ba, corner_bb, couplings):
    determinant = corner_aa * corner_bb - corner_ab * corner_ba
    corner_inverse = (
        jnp.stack(
            [jnp.stack([corner_bb, -corner_ab], -1), jnp.stack([-corner_ba, corner_aa], -1)], -2
        )
        / determinant[:, None, None]
    )
    blocks_count = corner_aa.shape[0]
    identity = jnp.eye(blocks_count, dtype=corner_inverse.dtype)
    diagonal_part = jnp.einsum("kab,kl->kalb", corner_inverse, identity, precision=highest).reshape(
        2 * blocks_count, 2 * blocks_count
    )
    link_values = jnp.zeros((2 * blocks_count - 1,), corner_inverse.dtype).at[1::2].set(-couplings)
    schur_matrix = diagonal_part + jnp.diag(link_values, 1) + jnp.diag(link_values, -1)
    return (corner_inverse, diagonal_part, jnp.linalg.cholesky(schur_matrix))


def make_solver(inverse_block, corner_rows, couplings, device_index, down_coupling, up_coupling):
    corner_inverse, diagonal_part, factor = interface_setup(
        corner_rows[:, 0], corner_rows[:, 1], corner_rows[:, 2], corner_rows[:, 3], couplings
    )
    block_len = inverse_block.shape[0]
    forward = lax.linalg.triangular_solve(factor, diagonal_part, left_side=True, lower=True)
    reach = lax.linalg.triangular_solve(
        factor, forward, left_side=True, lower=True, transpose_a=True
    )
    padded_reach = jnp.pad(reach, ((1, 1), (0, 0)))
    slice_rows = lax.dynamic_slice_in_dim(padded_reach, 2 * device_index, 4, 0)
    needed = jnp.stack([slice_rows[0], slice_rows[3]])

    def neighbours(end_values):
        zero_carry = jnp.zeros(end_values.shape, jnp.float32)
        nearby = zero_carry + jnp.dot(
            needed, lax.all_gather(end_values, "gz", axis=0, tiled=True), precision=highest
        )
        return (nearby[0], nearby[1])

    def solve(source):
        first_extent, second_extent, depth = source.shape
        line_count = first_extent * second_extent
        local_part = jnp.einsum("xyj,ij->xyi", source, inverse_block, precision=highest)
        end_values = jnp.stack(
            [
                local_part[:, :, 0].reshape(line_count),
                local_part[:, :, block_len - 1].reshape(line_count),
            ]
        )
        below_last, above_first = neighbours(end_values)
        return (
            local_part
            + (down_coupling * below_last).reshape(first_extent, second_extent, 1)
            * inverse_block[:, 0]
            + (up_coupling * above_first).reshape(first_extent, second_extent, 1)
            * inverse_block[:, block_len - 1]
        )

    return solve


def apply_operator(iterate, lateral_weight, down_faces, up_faces):
    padded = extended(iterate, (("gx", 0), ("gy", 1), ("gz", 2)), 1)
    lateral = (
        padded[:-2, 1:-1, 1:-1]
        + padded[2:, 1:-1, 1:-1]
        + padded[1:-1, :-2, 1:-1]
        + padded[1:-1, 2:, 1:-1]
    )
    return (
        lateral_weight * (4.0 * iterate - lateral)
        + down_faces * (iterate - padded[1:-1, 1:-1, :-2])
        + up_faces * (iterate - padded[1:-1, 1:-1, 2:])
    )


def restrict(field):
    first_extent, second_extent, depth = field.shape
    return field.reshape(first_extent // 2, 2, second_extent // 2, 2, depth).sum(axis=(1, 3)) * 0.25


def prolong(padded):
    first_extent = padded.shape[0] - 2
    second_extent = padded.shape[1] - 2
    depth = padded.shape[2]
    even_rows = 0.75 * padded[1:-1] + 0.25 * padded[:-2]
    odd_rows = 0.75 * padded[1:-1] + 0.25 * padded[2:]
    widened = jnp.stack([even_rows, odd_rows], 1).reshape(
        2 * first_extent, second_extent + 2, depth
    )
    even_rows = 0.75 * widened[:, 1:-1] + 0.25 * widened[:, :-2]
    odd_rows = 0.75 * widened[:, 1:-1] + 0.25 * widened[:, 2:]
    return jnp.stack([even_rows, odd_rows], 2).reshape(2 * first_extent, 2 * second_extent, depth)


def body(right_side, z_faces, xy_coupling, block_inverse):
    device_index = lax.axis_index("gz")
    levels_count = block_inverse.shape[0]
    last_cell = block_inverse.shape[1] - 1
    corner = jnp.stack(
        [
            block_inverse[:, 0, 0],
            block_inverse[:, 0, last_cell],
            block_inverse[:, last_cell, 0],
            block_inverse[:, last_cell, last_cell],
        ],
        -1,
    )[None]
    corners, firsts = (
        lax.all_gather(corner, "gz", axis=0, tiled=True),
        lax.all_gather(z_faces[:1], "gz", axis=0, tiled=True),
    )
    couplings = firsts[1:]
    edge_faces = jnp.concatenate([firsts, jnp.ones((1,), jnp.float32)])
    top_face = lax.dynamic_slice_in_dim(edge_faces, device_index + 1, 1, 0)
    up_faces = jnp.concatenate([z_faces[1:], top_face])
    solvers = [
        make_solver(
            block_inverse[level],
            corners[:, level],
            couplings,
            device_index,
            z_faces[0],
            top_face[0],
        )
        for level in range(levels_count)
    ]

    def operator(iterate, level):
        return apply_operator(iterate, xy_coupling[level], z_faces, up_faces)

    def multigrid_cycle(source, level):
        iterate = damping * solvers[level](source)
        iterate = iterate + damping * solvers[level](source - operator(iterate, level))
        if level == LEVELS - 1:
            return iterate
        coarse = multigrid_cycle(restrict(source - operator(iterate, level)), level + 1)
        widened = extended(coarse, (("gx", 0), ("gy", 1)), 1)
        iterate = iterate + prolong(widened)
        for sweep in range(SWEEPS):
            iterate = iterate + damping * solvers[level](source - operator(iterate, level))
        return iterate

    solution = multigrid_cycle(right_side, 0)
    return (solution, right_side - operator(solution, 0))


MESH = pl.DeviceIdType.MESH
HALOS = (4, 6, 6)
YPAD = 8


def block_range(offset, own, halo, extent):
    start = offset * own - halo
    low = max(0, start)
    high = min(extent, (offset + 1) * own + halo)
    return low, high - low, low - start


def cycle_kernel(geometry, f_ref, z_ref, e_ref, g_ref, sol_ref, res_ref, *scratch):
    gx_n, gy_n, gz_n, nx, ny, depth, levels = geometry
    (sinv, g_all, z_all, gather) = scratch[:4]
    R = scratch[4 : 4 + levels]
    U = scratch[4 + levels : 4 + 2 * levels]
    W = scratch[4 + 2 * levels : 4 + 3 * levels]
    V = scratch[4 + 3 * levels : 4 + 4 * levels]
    D = scratch[4 + 4 * levels : 4 + 5 * levels]
    (own1, own2, own3, c4u, c4d, c3u, c3d, cwu, cwd) = scratch[4 + 5 * levels : 13 + 5 * levels]
    OWN = (None, own1, own2, own3)
    (g_send, g_recv, h_send, h_recv, a_send, a_recv, o_send, o_recv) = scratch[13 + 5 * levels :]

    ix, iy, iz = lax.axis_index("gx"), lax.axis_index("gy"), lax.axis_index("gz")
    bx = ix * gz_n + iz
    bx_n = gx_n * gz_n
    f32 = jnp.float32

    def owned(level):
        return nx >> level, ny >> level

    def copy(src, dst, send, recv, device):
        return pltpu.make_async_remote_copy(
            src_ref=src,
            dst_ref=dst,
            send_sem=send,
            recv_sem=recv,
            device_id=device,
            device_id_type=MESH,
        )

    def setup_copies(other):
        here = (ix, iy, lax.rem(iz + other, gz_n))
        out = []
        for level in range(levels):
            out.append(
                copy(
                    g_ref.at[level],
                    g_all.at[level, iz],
                    g_send.at[other, level],
                    g_recv.at[other, level],
                    here,
                )
            )
        out.append(
            copy(z_ref, z_all.at[iz], g_send.at[other, levels], g_recv.at[other, levels], here)
        )
        return out

    def start_copies():
        out = []
        reach = -(-HALOS[0] // nx)
        for t in range(-reach, gz_n + reach):
            xs, xn, xd = block_range(t, nx, HALOS[0], nx * gz_n)
            dgx, target = t // gz_n, t % gz_n
            for dy in (-1, 0, 1):
                ys, yn, yd = block_range(dy, ny, YPAD, ny)
                out.append((t, dgx, target, dy, (xs, xn, xd), (ys, yn, yd)))
        return out

    plan0 = start_copies()

    def copy0(entry, source_z, device):
        t, dgx, target, dy, (xs, xn, xd), (ys, yn, yd) = entry
        slot = (t + gz_n) * 3 + dy + 1
        return copy(
            f_ref.at[pl.ds(xs, xn), pl.ds(ys, yn), :],
            R[0].at[pl.ds(xd, xn), source_z, pl.ds(yd, yn), :],
            h_send.at[0, slot],
            h_recv.at[0, slot, source_z],
            device,
        )

    def inside(x, y):
        return (x >= 0) & (x < gx_n) & (y >= 0) & (y < gy_n)

    def send0(start):
        for entry in plan0:
            t, dgx, target, dy = entry[:4]
            ok = inside(ix + dgx, iy + dy)
            if dgx == 0 and dy == 0:
                ok = ok & (iz != target)

            @pl.when(ok)
            def _():
                c = copy0(entry, iz, (ix + dgx, iy + dy, target))
                c.start() if start else c.wait_send()

    def recv0():
        for entry in plan0:
            t, dgx, target, dy = entry[:4]
            for source_z in range(gz_n):
                if dgx == 0 and dy == 0 and source_z == target:
                    continue

                @pl.when((iz == target) & inside(ix - dgx, iy - dy))
                def _():
                    copy0(entry, source_z, (ix - dgx, iy - dy, source_z)).wait_recv()

    reach_all = max(
        gz_n - 1 - (-HALOS[0] // nx), *[-(-HALOS[k] // owned(k)[0]) for k in (1, 2)]
    )
    barrier = pltpu.get_barrier_semaphore()

    def greet(other, count):
        x, y = other // gy_n, lax.rem(other, gy_n)
        near = (jnp.abs(x - bx) <= reach_all) & (jnp.abs(y - iy) <= 1)
        near = (near | (x == bx) | (y == iy)) & ((x != bx) | (y != iy))

        @pl.when(near)
        def _():
            pl.semaphore_signal(
                barrier,
                inc=1,
                device_id=(x // gz_n, y, lax.rem(x, gz_n)),
                device_id_type=MESH,
            )

        return count + jnp.where(near, 1, 0).astype(jnp.int32)

    partners = lax.fori_loop(0, bx_n * gy_n, greet, jnp.int32(0))


    for entry in plan0:
        t, dgx, target, dy, (xs, xn, xd) = entry[:5]
        if dgx == 0 and dy == 0:

            @pl.when(iz == target)
            def _():
                def step(i, _):
                    R[0][xd + i, target, pl.ds(YPAD, ny), :] = f_ref[xs + i]
                    return 0

                lax.fori_loop(0, xn, step, 0)

    for level in range(levels):
        g_all[level, iz] = g_ref[level]
    z_all[iz] = z_ref[...]

    for level in range(3):
        planes, zb, rows, lanes = R[level].shape
        halo = HALOS[level]
        n0, n1 = owned(level)
        reach = -(-halo // n0)
        for t in range(1, reach + 1):
            low = max(0, halo - t * n0)
            high = halo - (t - 1) * n0
            plane = jnp.zeros((high - low, zb, rows, lanes), f32)

            @pl.when(bx - t < 0)
            def _():
                R[level][low:high] = plane

            low2, high2 = planes - high, planes - low

            @pl.when(bx + t >= bx_n)
            def _():
                R[level][low2:high2] = plane

        edge = jnp.zeros((zb, YPAD, lanes), f32)

        @pl.when(iy == 0)
        def _():
            lax.fori_loop(0, planes, lambda i, c: zero_rows(R[level], i, 0, edge), 0)

        @pl.when(iy == gy_n - 1)
        def _():
            lax.fori_loop(0, planes, lambda i, c: zero_rows(R[level], i, rows - YPAD, edge), 0)

    def fill(ref):
        zero = jnp.zeros(ref.shape[1:], f32)

        def step(i, _):
            ref[i] = zero
            return 0

        lax.fori_loop(0, ref.shape[0], step, 0)

    for ref in (c4u, c4d, c3u, c3d, cwu, cwd):
        fill(ref)
    for level in range(levels):
        zero = jnp.zeros(W[level].shape[1:], f32)
        W[level][0] = zero
        W[level][W[level].shape[0] - 1] = zero

    pl.semaphore_wait(barrier, partners)
    send0(True)
    for other in range(1, gz_n):
        for c in setup_copies(other):
            c.start()

    for other in range(1, gz_n):
        for c in setup_copies(other):
            c.wait()

    def assemble(level, _):
        merged = g_all[level, 0]
        for k in range(1, gz_n):
            block = g_all[level, k]
            size, cz = merged.shape[0], block.shape[0]
            face = z_all[k][:, 0:1]
            a, d = block[0:1, 0:1], merged[size - 1 : size, size - 1 : size]
            last, first = merged[size - 1 : size], block[0:1]
            scale = face / (1.0 - face * face * a * d)
            p_row = jnp.concatenate([face * a * last, first], 1) * scale
            q_row = jnp.concatenate([last, face * d * first], 1) * scale
            top = jnp.concatenate([merged, jnp.zeros((size, cz), f32)], 1)
            low = jnp.concatenate([jnp.zeros((cz, size), f32), block], 1)
            top = top + merged[:, size - 1 : size] * p_row
            low = low + block[:, 0:1] * q_row
            merged = jnp.concatenate([top, low], 0)
        sinv[level] = (damping * merged).astype(jnp.bfloat16)
        return 0

    lax.fori_loop(0, levels, assemble, 0)

    def plane_mask(level, i):
        n0 = owned(level)[0]
        x = bx * n0 - HALOS[level] + i
        return jnp.where((x >= 0) & (x < bx_n * n0), 1.0, 0.0).astype(f32)

    def row_mask(level, rows, first, stride):
        n1 = owned(level)[1]
        y = lax.broadcasted_iota(jnp.int32, (rows, depth), 0) * stride + first
        y = y + iy * n1 - YPAD
        return jnp.where((y >= 0) & (y < gy_n * n1), 1.0, 0.0).astype(f32)

    def neighbours(level, i):
        centre = W[level][i + 1]
        rows = centre.shape[1]
        before = pltpu.roll(centre, 1, 1)
        after = pltpu.roll(centre, rows - 1, 1)
        if level > 2:
            y = lax.broadcasted_iota(jnp.int32, centre.shape, 1)
            before = jnp.where(y > 0, before, 0.0)
            after = jnp.where(y < rows - 1, after, 0.0)
        return centre, W[level][i] + W[level][i + 2] + before + after

    def sweep(level, first):
        planes, zb, rows, lanes = R[level].shape
        e = e_ref[level]
        chunk = planes
        while chunk % 2 == 0 and chunk * rows > 256:
            chunk //= 2

        def solve(s, _):
            at = s * chunk
            source = [R[level][pl.ds(at, chunk), k] for k in range(zb)]
            flat = [v.reshape(chunk * rows, lanes) for v in source]
            lhs = jnp.concatenate(flat, 1).astype(jnp.bfloat16)
            out = jnp.dot(lhs, sinv[level], preferred_element_type=f32)
            for k in range(zb):
                w = out[:, k * lanes : (k + 1) * lanes].reshape(chunk, rows, lanes)
                W[level][pl.ds(at + 1, chunk), k] = w
                U[level][pl.ds(at, chunk), k] = w if first else U[level][pl.ds(at, chunk), k] + w
                if level > 0:
                    dd = damping * source[k] - (4.0 * e) * w
                    D[level][pl.ds(at, chunk), k] = (
                        dd if first else D[level][pl.ds(at, chunk), k] + dd
                    )
            return 0

        lax.fori_loop(0, planes // chunk, solve, 0)

    def update(level):
        planes, zb, rows, lanes = R[level].shape
        e = e_ref[level]
        mask_y = row_mask(level, rows, 0, 1) if level < 3 else None

        def step(i, _):
            centre, total = neighbours(level, i)
            value = (1.0 - damping) * R[level][i] + e * total
            if level < 3:
                value = value * (mask_y * plane_mask(level, i))[None]
            R[level][i] = value
            return 0

        lax.fori_loop(0, planes, step, 0, unroll=2)

    def restrict_planes(level, dst, planes, x0, y0):
        rows = dst.shape[2]

        def step(j, _):
            for k in range(gz_n):
                total = None
                for a in (0, 1):
                    for b in (0, 1):
                        part = R[level][x0 + 2 * j + a, k, pl.ds(y0 + b, rows, 2), :]
                        total = part if total is None else total + part
                dst[j, k] = total * 0.25
            return 0

        lax.fori_loop(0, planes, step, 0)

    def prolong_planes(level, src, dst, offset, x0, y0):
        planes, zb, rows, lanes = R[level].shape
        half = rows // 2
        if level < 3:
            masks = [row_mask(level, half, b, 2) for b in (0, 1)]

        def step(j, _):
            for k in range(zb):
                def load(dx, dy):
                    return src[x0 + j + dx, k, pl.ds(y0 + dy, half), :]

                for b, dy in ((0, -1), (1, 1)):
                    mixed = [0.75 * load(dx, 0) + 0.25 * load(dx, dy) for dx in (-1, 0, 1)]
                    for a, far in ((0, 0), (1, 2)):
                        value = 0.75 * mixed[1] + 0.25 * mixed[far]
                        if level < 3:
                            value = value * (masks[b] * plane_mask(level, 2 * j + a))
                        dst[offset + 2 * j + a, k, pl.ds(b, half, 2), :] = value
            return 0

        lax.fori_loop(0, planes // 2, step, 0)

    def correct(level, coarse_u, coarse_d, x0, y0):
        planes = R[level].shape[0]
        rows = R[level].shape[2]
        e = e_ref[level]
        prolong_planes(level, coarse_u, W[level], 1, x0, y0)
        prolong_planes(level, coarse_d, V[level], 0, x0, y0)
        mask_y = row_mask(level, rows, 0, 1) if level < 3 else None

        def step(i, _):
            centre, total = neighbours(level, i)
            side = V[level][i]
            value = R[level][i] - side - (4.0 * e) * centre + e * total
            if level < 3:
                value = value * (mask_y * plane_mask(level, i))[None]
            R[level][i] = value
            U[level][i] = U[level][i] + centre
            if level > 0:
                D[level][i] = D[level][i] + side
            return 0

        lax.fori_loop(0, planes, step, 0)

    def exchange(level):
        n0, n1 = owned(level)
        halo = HALOS[level]
        own = OWN[level]
        reach = -(-halo // n0)
        window = R[level]

        def local(i, _):
            window[i + halo, :, pl.ds(YPAD, n1), :] = own[i]
            return 0

        def each(act):
            slot = 0
            for t in range(-reach, reach + 1):
                xs, xn, xd = block_range(t, n0, halo, n0)
                for dy in (-1, 0, 1):
                    if t == 0 and dy == 0:
                        continue
                    ys, yn, yd = block_range(dy, n1, YPAD, n1)
                    act(t, dy, (xs, xn, xd), (ys, yn, yd), slot)
                    slot += 1

        def build(t, dy, x, y, slot):
            there = bx + t + bx_n
            return copy(
                own.at[pl.ds(x[0], x[1]), :, pl.ds(y[0], y[1]), :],
                window.at[pl.ds(x[2], x[1]), :, pl.ds(y[2], y[1]), :],
                h_send.at[level, slot],
                h_recv.at[level, slot, 0],
                (there // gz_n - gx_n, iy + dy, lax.rem(there, gz_n)),
            )

        def valid(x, y):
            return (x >= 0) & (x < bx_n) & (y >= 0) & (y < gy_n)

        def start(t, dy, x, y, slot):
            @pl.when(valid(bx + t, iy + dy))
            def _():
                build(t, dy, x, y, slot).start()

        def finish(t, dy, x, y, slot):
            @pl.when(valid(bx - t, iy - dy))
            def _():
                build(t, dy, x, y, slot).wait_recv()

        def drain(t, dy, x, y, slot):
            @pl.when(valid(bx + t, iy + dy))
            def _():
                build(t, dy, x, y, slot).wait_send()

        each(start)
        lax.fori_loop(0, n0, local, 0)
        each(finish)
        return lambda: each(drain)

    def gather_all():
        def line_y(other, slot):
            return copy(
                own3,
                gather.at[bx, slot],
                a_send.at[0, other],
                a_recv.at[0, slot],
                (ix, other, iz),
            )

        def line_x(other, slot):
            return copy(
                gather.at[slot],
                gather.at[slot],
                a_send.at[1, other],
                a_recv.at[1, slot],
                (other // gz_n, iy, lax.rem(other, gz_n)),
            )

        def over(build, me, count, act):
            for s in range(1, count):
                act(build, lax.rem(me + s, count), me)

        def start(build, other, me):
            build(other, me).start()

        def finish(build, other, me):
            build(other, other).wait_recv()

        def drain(build, other, me):
            build(other, me).wait_send()

        over(line_y, iy, gy_n, start)
        gather[bx, iy] = own3[...]
        over(line_y, iy, gy_n, finish)
        over(line_x, bx, bx_n, start)
        over(line_x, bx, bx_n, finish)
        n0, n1 = owned(3)

        def place(b, _):
            for i in range(n0):
                for y in range(gy_n):
                    R[3][b * n0 + i, :, pl.ds(y * n1, n1), :] = gather[b, y, i]
            return 0

        lax.fori_loop(0, bx_n, place, 0)

        def drains():
            over(line_y, iy, gy_n, drain)
            over(line_x, bx, bx_n, drain)

        return drains

    def store_padded(level, src, dst, x0):
        rows = src.shape[2]

        def step(i, _):
            dst[x0 + i, :, pl.ds(YPAD, rows), :] = src[i]
            return 0

        lax.fori_loop(0, src.shape[0], step, 0)

    recv0()
    drains = [lambda: send0(False)]
    for level in range(3):
        sweep(level, True)
        update(level)
        sweep(level, False)
        update(level)
        n0 = owned(level + 1)[0]
        restrict_planes(level, OWN[level + 1], n0, HALOS[level], YPAD)
        drains.append(exchange(level + 1) if level < 2 else gather_all())
    sweep(3, True)
    update(3)
    sweep(3, False)
    update(3)
    restrict_planes(3, R[4], R[4].shape[0], 0, 0)
    sweep(4, True)
    update(4)
    sweep(4, False)
    store_padded(4, U[4], c4u, 1)
    store_padded(4, D[4], c4d, 1)
    correct(3, c4u, c4d, 1, YPAD)
    sweep(3, False)
    update(3)
    sweep(3, False)
    pad3 = HALOS[2] // 2 + 1
    store_padded(3, U[3], c3u, pad3)
    store_padded(3, D[3], c3d, pad3)
    n0, n1 = owned(3)
    margin = YPAD // 2
    for y in range(gy_n):

        @pl.when(iy == y)
        def _():
            def step(j, _):
                for src, dst in ((c3u, cwu), (c3d, cwd)):
                    dst[j, :, pl.ds(margin, n1 + 4 * margin), :] = src[
                        bx * n0 + j, :, pl.ds(y * n1, n1 + 4 * margin), :
                    ]
                return 0

            lax.fori_loop(0, cwu.shape[0], step, 0)

    for level in (2, 1, 0):
        if level == 2:
            correct(2, cwu, cwd, 1, YPAD)
        else:
            x0 = HALOS[level + 1] - HALOS[level] // 2
            correct(level, U[level + 1], D[level + 1], x0, YPAD // 2)
        sweep(level, False)
        update(level)
        sweep(level, False)

    def out_copies(which):
        src, dst = ((U[0], sol_ref), (R[0], res_ref))[which]
        out = []
        for other in range(1, gz_n):
            there = lax.rem(iz + other, gz_n)
            out.append(
                copy(
                    src.at[pl.ds(HALOS[0], nx), there, pl.ds(YPAD, ny), :],
                    dst.at[pl.ds(iz * nx, nx), :, :],
                    o_send.at[which, other],
                    o_recv.at[which, other],
                    (ix, iy, there),
                )
            )
        return out

    def out_local(which):
        src, dst = ((U[0], sol_ref), (R[0], res_ref))[which]

        def step(i, _):
            dst[iz * nx + i] = src[HALOS[0] + i, iz, pl.ds(YPAD, ny), :]
            return 0

        lax.fori_loop(0, nx, step, 0)

    for c in out_copies(0):
        c.start()
    update(0)
    for c in out_copies(1):
        c.start()
    out_local(0)
    out_local(1)
    for drain in drains:
        drain()
    for which in (0, 1):
        for c in out_copies(which):
            c.wait()


def zero_rows(ref, i, at, value):
    ref[i, :, pl.ds(at, YPAD), :] = value
    return 0


def fits(mesh, shape, inverse_shape):
    gx_n, gy_n, gz_n = (mesh.shape[a] for a in ("gx", "gy", "gz"))
    nx, ny = shape[0] // (gx_n * gz_n), shape[1] // gy_n
    return (
        inverse_shape[0] == LEVELS == 5
        and SWEEPS == 2
        and inverse_shape[2] == 128
        and nx % 8 == 0
        and ny % 32 == 0
        and (shape[1] >> 4) % 8 == 0
        and gz_n <= 2
    )


def fused_body(mesh, right_side, z_faces, xy_coupling, block_inverse):
    gx_n, gy_n, gz_n = (mesh.shape[a] for a in ("gx", "gy", "gz"))
    levels, _, depth = block_inverse.shape
    nx, ny = right_side.shape[0] // gz_n, right_side.shape[1]
    windows = []
    for level in range(levels):
        if level < 3:
            size = ((nx >> level) + 2 * HALOS[level], (ny >> level) + 2 * YPAD)
        else:
            size = ((nx * gx_n * gz_n) >> level, (ny * gy_n) >> level)
        windows.append((size[0], gz_n, size[1], depth))
    vmem = lambda shape: pltpu.VMEM(shape, jnp.float32)
    full3, full4 = windows[3], windows[4]
    pad3 = HALOS[2] // 2 + 1
    c4 = (full4[0] + 2, gz_n, full4[2] + 2 * YPAD, depth)
    c3 = (full3[0] + 2 * pad3, gz_n, full3[2] + 2 * YPAD, depth)
    cw = (windows[2][0] // 2 + 2, gz_n, (ny >> 3) + 20, depth)
    reach = 2 * max(-(-HALOS[k] // (nx >> k)) for k in range(3)) + 1
    slots = 3 * max(reach, 3 * gz_n + 1)
    dma = pltpu.SemaphoreType.DMA
    own = lambda k: (nx >> k, gz_n, ny >> k, depth)
    scratch = (
        [
            pltpu.VMEM((levels, gz_n * depth, gz_n * depth), jnp.bfloat16),
            vmem((levels, gz_n, depth, depth)),
            vmem((gz_n, 1, depth)),
            vmem((gx_n * gz_n, gy_n) + own(3)),
        ]
        + [vmem(w) for w in windows]
        + [vmem(w) for w in windows]
        + [vmem((w[0] + 2,) + w[1:]) for w in windows]
        + [vmem(w) for w in windows]
        + [vmem(w) for w in windows]
        + [vmem(own(1)), vmem(own(2)), vmem(own(3))]
        + [vmem(c4), vmem(c4), vmem(c3), vmem(c3), vmem(cw), vmem(cw)]
        + [dma((gz_n, levels + 1))] * 2
        + [dma((3, slots)), dma((3, slots, gz_n))]
        + [dma((2, max(gx_n * gz_n, gy_n)))] * 2
        + [dma((2, gz_n))] * 2
    )
    in_vmem = pl.BlockSpec(memory_space=pltpu.VMEM)
    return tuple(
        pl.pallas_call(
            functools.partial(cycle_kernel, (gx_n, gy_n, gz_n, nx, ny, depth, levels)),
            out_shape=[jax.ShapeDtypeStruct(right_side.shape, jnp.float32)] * 2,
            in_specs=[
                in_vmem,
                in_vmem,
                pl.BlockSpec(memory_space=pltpu.SMEM),
                in_vmem,
            ],
            out_specs=[in_vmem, in_vmem],
            scratch_shapes=scratch,
            compiler_params=pltpu.CompilerParams(
                collective_id=0, has_side_effects=True, vmem_limit_bytes=60 * 1024 * 1024
            ),
        )(right_side, z_faces.reshape(1, -1), xy_coupling, block_inverse)
    )


def solution(mesh):
    def call(right_side, z_faces, xy_coupling, block_inverse):
        local = body
        if fits(mesh, right_side.shape, block_inverse.shape):
            local = functools.partial(fused_body, mesh)
        return jax.shard_map(
            local,
            mesh=mesh,
            in_specs=(P("gx", "gy", "gz"), P("gz"), P(), P(None, "gz", None)),
            out_specs=(P("gx", "gy", "gz"), P("gx", "gy", "gz")),
            check_vma=False,
        )(right_side, z_faces, xy_coupling, block_inverse)

    return call
```

```python
import functools

import jax
import jax.numpy as jnp
from jax import lax
from jax.experimental import pallas as pl
from jax.experimental.pallas import tpu as pltpu
from jax.sharding import PartitionSpec as P

LEVELS = 5
SWEEPS = 2


damping = 0.8
highest = lax.Precision.HIGHEST


def extended(cells, sides, width):
    for axis, dim in sides:
        count = lax.axis_size(axis)
        ends = count - 1
        head = lax.slice_in_dim(cells, 0, width, axis=dim)
        tail = lax.slice_in_dim(cells, cells.shape[dim] - width, cells.shape[dim], axis=dim)
        cells = jnp.concatenate(
            [
                lax.ppermute(tail, axis, [(i, (i + 1) % count) for i in range(ends)]),
                cells,
                lax.ppermute(head, axis, [((i + 1) % count, i) for i in range(ends)]),
            ],
            axis=dim,
        )
    return cells


def interface_setup(corner_aa, corner_ab, corner_ba, corner_bb, couplings):
    determinant = corner_aa * corner_bb - corner_ab * corner_ba
    corner_inverse = (
        jnp.stack(
            [jnp.stack([corner_bb, -corner_ab], -1), jnp.stack([-corner_ba, corner_aa], -1)], -2
        )
        / determinant[:, None, None]
    )
    blocks_count = corner_aa.shape[0]
    identity = jnp.eye(blocks_count, dtype=corner_inverse.dtype)
    diagonal_part = jnp.einsum("kab,kl->kalb", corner_inverse, identity, precision=highest).reshape(
        2 * blocks_count, 2 * blocks_count
    )
    link_values = jnp.zeros((2 * blocks_count - 1,), corner_inverse.dtype).at[1::2].set(-couplings)
    schur_matrix = diagonal_part + jnp.diag(link_values, 1) + jnp.diag(link_values, -1)
    return (corner_inverse, diagonal_part, jnp.linalg.cholesky(schur_matrix))


def make_solver(inverse_block, corner_rows, couplings, device_index, down_coupling, up_coupling):
    corner_inverse, diagonal_part, factor = interface_setup(
        corner_rows[:, 0], corner_rows[:, 1], corner_rows[:, 2], corner_rows[:, 3], couplings
    )
    block_len = inverse_block.shape[0]
    forward = lax.linalg.triangular_solve(factor, diagonal_part, left_side=True, lower=True)
    reach = lax.linalg.triangular_solve(
        factor, forward, left_side=True, lower=True, transpose_a=True
    )
    padded_reach = jnp.pad(reach, ((1, 1), (0, 0)))
    slice_rows = lax.dynamic_slice_in_dim(padded_reach, 2 * device_index, 4, 0)
    needed = jnp.stack([slice_rows[0], slice_rows[3]])

    def neighbours(end_values):
        zero_carry = jnp.zeros(end_values.shape, jnp.float32)
        nearby = zero_carry + jnp.dot(
            needed, lax.all_gather(end_values, "gz", axis=0, tiled=True), precision=highest
        )
        return (nearby[0], nearby[1])

    def solve(source):
        first_extent, second_extent, depth = source.shape
        line_count = first_extent * second_extent
        local_part = jnp.einsum("xyj,ij->xyi", source, inverse_block, precision=highest)
        end_values = jnp.stack(
            [
                local_part[:, :, 0].reshape(line_count),
                local_part[:, :, block_len - 1].reshape(line_count),
            ]
        )
        below_last, above_first = neighbours(end_values)
        return (
            local_part
            + (down_coupling * below_last).reshape(first_extent, second_extent, 1)
            * inverse_block[:, 0]
            + (up_coupling * above_first).reshape(first_extent, second_extent, 1)
            * inverse_block[:, block_len - 1]
        )

    return solve


def apply_operator(iterate, lateral_weight, down_faces, up_faces):
    padded = extended(iterate, (("gx", 0), ("gy", 1), ("gz", 2)), 1)
    lateral = (
        padded[:-2, 1:-1, 1:-1]
        + padded[2:, 1:-1, 1:-1]
        + padded[1:-1, :-2, 1:-1]
        + padded[1:-1, 2:, 1:-1]
    )
    return (
        lateral_weight * (4.0 * iterate - lateral)
        + down_faces * (iterate - padded[1:-1, 1:-1, :-2])
        + up_faces * (iterate - padded[1:-1, 1:-1, 2:])
    )


def restrict(field):
    first_extent, second_extent, depth = field.shape
    return field.reshape(first_extent // 2, 2, second_extent // 2, 2, depth).sum(axis=(1, 3)) * 0.25


def prolong(padded):
    first_extent = padded.shape[0] - 2
    second_extent = padded.shape[1] - 2
    depth = padded.shape[2]
    even_rows = 0.75 * padded[1:-1] + 0.25 * padded[:-2]
    odd_rows = 0.75 * padded[1:-1] + 0.25 * padded[2:]
    widened = jnp.stack([even_rows, odd_rows], 1).reshape(
        2 * first_extent, second_extent + 2, depth
    )
    even_rows = 0.75 * widened[:, 1:-1] + 0.25 * widened[:, :-2]
    odd_rows = 0.75 * widened[:, 1:-1] + 0.25 * widened[:, 2:]
    return jnp.stack([even_rows, odd_rows], 2).reshape(2 * first_extent, 2 * second_extent, depth)


def body(right_side, z_faces, xy_coupling, block_inverse):
    device_index = lax.axis_index("gz")
    levels_count = block_inverse.shape[0]
    last_cell = block_inverse.shape[1] - 1
    corner = jnp.stack(
        [
            block_inverse[:, 0, 0],
            block_inverse[:, 0, last_cell],
            block_inverse[:, last_cell, 0],
            block_inverse[:, last_cell, last_cell],
        ],
        -1,
    )[None]
    corners, firsts = (
        lax.all_gather(corner, "gz", axis=0, tiled=True),
        lax.all_gather(z_faces[:1], "gz", axis=0, tiled=True),
    )
    couplings = firsts[1:]
    edge_faces = jnp.concatenate([firsts, jnp.ones((1,), jnp.float32)])
    top_face = lax.dynamic_slice_in_dim(edge_faces, device_index + 1, 1, 0)
    up_faces = jnp.concatenate([z_faces[1:], top_face])
    solvers = [
        make_solver(
            block_inverse[level],
            corners[:, level],
            couplings,
            device_index,
            z_faces[0],
            top_face[0],
        )
        for level in range(levels_count)
    ]

    def operator(iterate, level):
        return apply_operator(iterate, xy_coupling[level], z_faces, up_faces)

    def multigrid_cycle(source, level):
        iterate = damping * solvers[level](source)
        iterate = iterate + damping * solvers[level](source - operator(iterate, level))
        if level == LEVELS - 1:
            return iterate
        coarse = multigrid_cycle(restrict(source - operator(iterate, level)), level + 1)
        widened = extended(coarse, (("gx", 0), ("gy", 1)), 1)
        iterate = iterate + prolong(widened)
        for sweep in range(SWEEPS):
            iterate = iterate + damping * solvers[level](source - operator(iterate, level))
        return iterate

    solution = multigrid_cycle(right_side, 0)
    return (solution, right_side - operator(solution, 0))


MESH = pl.DeviceIdType.MESH
HALOS = (4, 6, 6)
ROWS = (4, 5, 6)
YPAD = 8


def block_range(offset, own, halo, extent):
    start = offset * own - halo
    low = max(0, start)
    high = min(extent, (offset + 1) * own + halo)
    return low, high - low, low - start


def cycle_kernel(geometry, f_ref, z_ref, e_ref, g_ref, sol_ref, res_ref, *scratch):
    gx_n, gy_n, gz_n, nx, ny, depth, levels = geometry
    (sinv, g_all, z_all, gather) = scratch[:4]
    R = scratch[4 : 4 + levels]
    U = scratch[4 + levels : 4 + 2 * levels]
    W = scratch[4 + 2 * levels : 4 + 3 * levels]
    V = scratch[4 + 3 * levels : 4 + 4 * levels]
    D = scratch[4 + 4 * levels : 4 + 5 * levels]
    (own1, own2, own3, c4u, c4d, c3u, c3d, cwu, cwd) = scratch[4 + 5 * levels : 13 + 5 * levels]
    OWN = (None, own1, own2, own3)
    (g_send, g_recv, h_send, h_recv, a_send, a_recv, o_send, o_recv) = scratch[13 + 5 * levels :]

    ix, iy, iz = lax.axis_index("gx"), lax.axis_index("gy"), lax.axis_index("gz")
    bx = ix * gz_n + iz
    bx_n = gx_n * gz_n
    f32 = jnp.float32

    def owned(level):
        return nx >> level, ny >> level

    def copy(src, dst, send, recv, device):
        return pltpu.make_async_remote_copy(
            src_ref=src,
            dst_ref=dst,
            send_sem=send,
            recv_sem=recv,
            device_id=device,
            device_id_type=MESH,
        )

    def setup_copies(other):
        here = (ix, iy, lax.rem(iz + other, gz_n))
        out = []
        for level in range(levels):
            out.append(
                copy(
                    g_ref.at[level],
                    g_all.at[level, iz],
                    g_send.at[other, level],
                    g_recv.at[other, level],
                    here,
                )
            )
        out.append(
            copy(z_ref, z_all.at[iz], g_send.at[other, levels], g_recv.at[other, levels], here)
        )
        return out

    def start_copies():
        out = []
        reach = -(-HALOS[0] // nx)
        for t in range(-reach, gz_n + reach):
            xs, xn, xd = block_range(t, nx, HALOS[0], nx * gz_n)
            dgx, target = t // gz_n, t % gz_n
            for dy in (-1, 0, 1):
                ys, yn, yd = block_range(dy, ny, ROWS[0], ny)
                yd += YPAD - ROWS[0]
                out.append((t, dgx, target, dy, (xs, xn, xd), (ys, yn, yd)))
        return out

    plan0 = start_copies()

    def copy0(entry, source_z, device):
        t, dgx, target, dy, (xs, xn, xd), (ys, yn, yd) = entry
        slot = (t + gz_n) * 3 + dy + 1
        return copy(
            f_ref.at[pl.ds(xs, xn), pl.ds(ys, yn), :],
            R[0].at[pl.ds(xd, xn), source_z, pl.ds(yd, yn), :],
            h_send.at[0, slot],
            h_recv.at[0, slot, source_z],
            device,
        )

    def inside(x, y):
        return (x >= 0) & (x < gx_n) & (y >= 0) & (y < gy_n)

    def send0(start):
        for entry in plan0:
            t, dgx, target, dy = entry[:4]
            ok = inside(ix + dgx, iy + dy)
            if dgx == 0 and dy == 0:
                ok = ok & (iz != target)

            @pl.when(ok)
            def _():
                c = copy0(entry, iz, (ix + dgx, iy + dy, target))
                c.start() if start else c.wait_send()

    def recv0():
        for entry in plan0:
            t, dgx, target, dy = entry[:4]
            for source_z in range(gz_n):
                if dgx == 0 and dy == 0 and source_z == target:
                    continue

                @pl.when((iz == target) & inside(ix - dgx, iy - dy))
                def _():
                    copy0(entry, source_z, (ix - dgx, iy - dy, source_z)).wait_recv()

    reach_all = max(
        gz_n - 1 - (-HALOS[0] // nx), *[-(-HALOS[k] // owned(k)[0]) for k in (1, 2)]
    )
    barrier = pltpu.get_barrier_semaphore()

    def greet(other, count):
        x, y = other // gy_n, lax.rem(other, gy_n)
        near = (jnp.abs(x - bx) <= reach_all) & (jnp.abs(y - iy) <= 1)
        near = (near | (x == bx) | (y == iy)) & ((x != bx) | (y != iy))

        @pl.when(near)
        def _():
            pl.semaphore_signal(
                barrier,
                inc=1,
                device_id=(x // gz_n, y, lax.rem(x, gz_n)),
                device_id_type=MESH,
            )

        return count + jnp.where(near, 1, 0).astype(jnp.int32)

    partners = lax.fori_loop(0, bx_n * gy_n, greet, jnp.int32(0))


    for entry in plan0:
        t, dgx, target, dy, (xs, xn, xd) = entry[:5]
        if dgx == 0 and dy == 0:

            @pl.when(iz == target)
            def _():
                def step(i, _):
                    R[0][xd + i, target, pl.ds(YPAD, ny), :] = f_ref[xs + i]
                    return 0

                lax.fori_loop(0, xn, step, 0)

    for level in range(levels):
        g_all[level, iz] = g_ref[level]
    z_all[iz] = z_ref[...]

    for level in range(3):
        planes, zb, rows, lanes = R[level].shape
        halo = HALOS[level]
        n0, n1 = owned(level)
        reach = -(-halo // n0)
        for t in range(1, reach + 1):
            low = max(0, halo - t * n0)
            high = halo - (t - 1) * n0
            plane = jnp.zeros((high - low, zb, rows, lanes), f32)

            @pl.when(bx - t < 0)
            def _():
                R[level][low:high] = plane

            low2, high2 = planes - high, planes - low

            @pl.when(bx + t >= bx_n)
            def _():
                R[level][low2:high2] = plane

        spare = jnp.zeros((zb, YPAD - ROWS[level], lanes), f32)

        def outer(i, _):
            R[level][i, :, pl.ds(0, YPAD - ROWS[level])] = spare
            R[level][i, :, pl.ds(rows - YPAD + ROWS[level], YPAD - ROWS[level])] = spare
            return 0

        lax.fori_loop(0, planes, outer, 0)
        edge = jnp.zeros((zb, YPAD, lanes), f32)

        @pl.when(iy == 0)
        def _():
            lax.fori_loop(0, planes, lambda i, c: zero_rows(R[level], i, 0, edge), 0)

        @pl.when(iy == gy_n - 1)
        def _():
            lax.fori_loop(0, planes, lambda i, c: zero_rows(R[level], i, rows - YPAD, edge), 0)

    def fill(ref):
        zero = jnp.zeros(ref.shape[1:], f32)

        def step(i, _):
            ref[i] = zero
            return 0

        lax.fori_loop(0, ref.shape[0], step, 0)

    for ref in (c4u, c4d, c3u, c3d, cwu, cwd):
        fill(ref)
    for level in range(levels):
        zero = jnp.zeros(W[level].shape[1:], f32)
        W[level][0] = zero
        W[level][W[level].shape[0] - 1] = zero

    pl.semaphore_wait(barrier, partners)
    send0(True)
    for other in range(1, gz_n):
        for c in setup_copies(other):
            c.start()

    for other in range(1, gz_n):
        for c in setup_copies(other):
            c.wait()

    def assemble(level, _):
        merged = g_all[level, 0]
        for k in range(1, gz_n):
            block = g_all[level, k]
            size, cz = merged.shape[0], block.shape[0]
            face = z_all[k][:, 0:1]
            a, d = block[0:1, 0:1], merged[size - 1 : size, size - 1 : size]
            last, first = merged[size - 1 : size], block[0:1]
            scale = face / (1.0 - face * face * a * d)
            p_row = jnp.concatenate([face * a * last, first], 1) * scale
            q_row = jnp.concatenate([last, face * d * first], 1) * scale
            top = jnp.concatenate([merged, jnp.zeros((size, cz), f32)], 1)
            low = jnp.concatenate([jnp.zeros((cz, size), f32), block], 1)
            top = top + merged[:, size - 1 : size] * p_row
            low = low + block[:, 0:1] * q_row
            merged = jnp.concatenate([top, low], 0)
        sinv[level] = (damping * merged).astype(jnp.bfloat16)
        return 0

    lax.fori_loop(0, levels, assemble, 0)

    def plane_mask(level, i):
        n0 = owned(level)[0]
        x = bx * n0 - HALOS[level] + i
        return jnp.where((x >= 0) & (x < bx_n * n0), 1.0, 0.0).astype(f32)

    def row_mask(level, rows, first, stride):
        n1 = owned(level)[1]
        y = lax.broadcasted_iota(jnp.int32, (rows, depth), 0) * stride + first
        y = y + iy * n1 - YPAD
        return jnp.where((y >= 0) & (y < gy_n * n1), 1.0, 0.0).astype(f32)

    def neighbours(level, i):
        centre = W[level][i + 1]
        rows = centre.shape[1]
        before = pltpu.roll(centre, 1, 1)
        after = pltpu.roll(centre, rows - 1, 1)
        if level > 2:
            y = lax.broadcasted_iota(jnp.int32, centre.shape, 1)
            before = jnp.where(y > 0, before, 0.0)
            after = jnp.where(y < rows - 1, after, 0.0)
        return centre, W[level][i] + W[level][i + 2] + before + after

    def sweep(level, first, margin=0):
        planes, zb, rows, lanes = R[level].shape
        e = e_ref[level]

        def widest(count):
            return max(c for c in range(1, count + 1) if count % c == 0 and c * rows <= 300)

        while margin and widest(planes - 2 * margin) * rows < 160:
            margin -= 1
        chunk = widest(planes - 2 * margin)

        def solve(s, _):
            at = margin + s * chunk
            source = [R[level][pl.ds(at, chunk), k] for k in range(zb)]
            flat = [v.reshape(chunk * rows, lanes) for v in source]
            lhs = jnp.concatenate(flat, 1).astype(jnp.bfloat16)
            out = jnp.dot(lhs, sinv[level], preferred_element_type=f32)
            for k in range(zb):
                w = out[:, k * lanes : (k + 1) * lanes].reshape(chunk, rows, lanes)
                W[level][pl.ds(at + 1, chunk), k] = w
                U[level][pl.ds(at, chunk), k] = w if first else U[level][pl.ds(at, chunk), k] + w
                if level > 0:
                    dd = damping * source[k] - (4.0 * e) * w
                    D[level][pl.ds(at, chunk), k] = (
                        dd if first else D[level][pl.ds(at, chunk), k] + dd
                    )
            return 0

        lax.fori_loop(0, (planes - 2 * margin) // chunk, solve, 0)

    def update(level, margin=0):
        planes, zb, rows, lanes = R[level].shape
        e = e_ref[level]
        mask_y = row_mask(level, rows, 0, 1) if level < 3 else None

        def step(i, _):
            centre, total = neighbours(level, i)
            value = (1.0 - damping) * R[level][i] + e * total
            if level < 3:
                value = value * (mask_y * plane_mask(level, i))[None]
            R[level][i] = value
            return 0

        lax.fori_loop(margin, planes - margin, step, 0, unroll=2)

    def restrict_planes(level, dst, planes, x0, y0):
        rows = dst.shape[2]

        def step(j, _):
            for k in range(gz_n):
                total = None
                for a in (0, 1):
                    for b in (0, 1):
                        part = R[level][x0 + 2 * j + a, k, pl.ds(y0 + b, rows, 2), :]
                        total = part if total is None else total + part
                dst[j, k] = total * 0.25
            return 0

        lax.fori_loop(0, planes, step, 0)

    def prolong_planes(level, src, dst, offset, x0, y0):
        planes, zb, rows, lanes = R[level].shape
        half = rows // 2
        if level < 3:
            masks = [row_mask(level, half, b, 2) for b in (0, 1)]

        def step(j, _):
            for k in range(zb):
                def load(dx, dy):
                    return src[x0 + j + dx, k, pl.ds(y0 + dy, half), :]

                for b, dy in ((0, -1), (1, 1)):
                    mixed = [0.75 * load(dx, 0) + 0.25 * load(dx, dy) for dx in (-1, 0, 1)]
                    for a, far in ((0, 0), (1, 2)):
                        value = 0.75 * mixed[1] + 0.25 * mixed[far]
                        if level < 3:
                            value = value * (masks[b] * plane_mask(level, 2 * j + a))
                        dst[offset + 2 * j + a, k, pl.ds(b, half, 2), :] = value
            return 0

        lax.fori_loop(0, planes // 2, step, 0)

    def correct(level, coarse_u, coarse_d, x0, y0, margin=0):
        planes = R[level].shape[0]
        rows = R[level].shape[2]
        e = e_ref[level]
        prolong_planes(level, coarse_u, W[level], 1, x0, y0)
        prolong_planes(level, coarse_d, V[level], 0, x0, y0)
        mask_y = row_mask(level, rows, 0, 1) if level < 3 else None

        def step(i, _):
            centre, total = neighbours(level, i)
            side = V[level][i]
            value = R[level][i] - side - (4.0 * e) * centre + e * total
            if level < 3:
                value = value * (mask_y * plane_mask(level, i))[None]
            R[level][i] = value
            U[level][i] = U[level][i] + centre
            if level > 0:
                D[level][i] = D[level][i] + side
            return 0

        lax.fori_loop(margin, planes - margin, step, 0)

    def exchange(level):
        n0, n1 = owned(level)
        halo = HALOS[level]
        own = OWN[level]
        reach = -(-halo // n0)
        window = R[level]

        def local(i, _):
            window[i + halo, :, pl.ds(YPAD, n1), :] = own[i]
            return 0

        def each(act):
            slot = 0
            for t in range(-reach, reach + 1):
                xs, xn, xd = block_range(t, n0, halo, n0)
                for dy in (-1, 0, 1):
                    if t == 0 and dy == 0:
                        continue
                    ys, yn, yd = block_range(dy, n1, ROWS[level], n1)
                    yd += YPAD - ROWS[level]
                    act(t, dy, (xs, xn, xd), (ys, yn, yd), slot)
                    slot += 1

        def build(t, dy, x, y, slot):
            there = bx + t + bx_n
            return copy(
                own.at[pl.ds(x[0], x[1]), :, pl.ds(y[0], y[1]), :],
                window.at[pl.ds(x[2], x[1]), :, pl.ds(y[2], y[1]), :],
                h_send.at[level, slot],
                h_recv.at[level, slot, 0],
                (there // gz_n - gx_n, iy + dy, lax.rem(there, gz_n)),
            )

        def valid(x, y):
            return (x >= 0) & (x < bx_n) & (y >= 0) & (y < gy_n)

        def start(t, dy, x, y, slot):
            @pl.when(valid(bx + t, iy + dy))
            def _():
                build(t, dy, x, y, slot).start()

        def finish(t, dy, x, y, slot):
            @pl.when(valid(bx - t, iy - dy))
            def _():
                build(t, dy, x, y, slot).wait_recv()

        def drain(t, dy, x, y, slot):
            @pl.when(valid(bx + t, iy + dy))
            def _():
                build(t, dy, x, y, slot).wait_send()

        each(start)
        lax.fori_loop(0, n0, local, 0)
        each(finish)
        return lambda: each(drain)

    def gather_all():
        def line_y(other, slot):
            return copy(
                own3,
                gather.at[bx, slot],
                a_send.at[0, other],
                a_recv.at[0, slot],
                (ix, other, iz),
            )

        def line_x(other, slot):
            return copy(
                gather.at[slot],
                gather.at[slot],
                a_send.at[1, other],
                a_recv.at[1, slot],
                (other // gz_n, iy, lax.rem(other, gz_n)),
            )

        def over(build, me, count, act):
            for s in range(1, count):
                act(build, lax.rem(me + s, count), me)

        def start(build, other, me):
            build(other, me).start()

        def finish(build, other, me):
            build(other, other).wait_recv()

        def drain(build, other, me):
            build(other, me).wait_send()

        over(line_y, iy, gy_n, start)
        gather[bx, iy] = own3[...]
        over(line_y, iy, gy_n, finish)
        over(line_x, bx, bx_n, start)
        over(line_x, bx, bx_n, finish)
        n0, n1 = owned(3)

        def place(b, _):
            for i in range(n0):
                for y in range(gy_n):
                    R[3][b * n0 + i, :, pl.ds(y * n1, n1), :] = gather[b, y, i]
            return 0

        lax.fori_loop(0, bx_n, place, 0)

        def drains():
            over(line_y, iy, gy_n, drain)
            over(line_x, bx, bx_n, drain)

        return drains

    def store_padded(level, src, dst, x0):
        rows = src.shape[2]

        def step(i, _):
            dst[x0 + i, :, pl.ds(YPAD, rows), :] = src[i]
            return 0

        lax.fori_loop(0, src.shape[0], step, 0)

    recv0()
    drains = [lambda: send0(False)]
    for level in range(3):
        slack = HALOS[level] - ROWS[level]
        sweep(level, True)
        update(level, slack + 1)
        sweep(level, False, slack + 1)
        update(level, slack + 2)
        n0 = owned(level + 1)[0]
        restrict_planes(level, OWN[level + 1], n0, HALOS[level], YPAD)
        drains.append(exchange(level + 1) if level < 2 else gather_all())
    sweep(3, True)
    update(3)
    sweep(3, False)
    update(3)
    restrict_planes(3, R[4], R[4].shape[0], 0, 0)
    sweep(4, True)
    update(4)
    sweep(4, False)
    store_padded(4, U[4], c4u, 1)
    store_padded(4, D[4], c4d, 1)
    correct(3, c4u, c4d, 1, YPAD)
    sweep(3, False)
    update(3)
    sweep(3, False)
    pad3 = HALOS[2] // 2 + 1
    store_padded(3, U[3], c3u, pad3)
    store_padded(3, D[3], c3d, pad3)
    n0, n1 = owned(3)
    margin = YPAD // 2
    for y in range(gy_n):

        @pl.when(iy == y)
        def _():
            def step(j, _):
                for src, dst in ((c3u, cwu), (c3d, cwd)):
                    dst[j, :, pl.ds(margin, n1 + 4 * margin), :] = src[
                        bx * n0 + j, :, pl.ds(y * n1, n1 + 4 * margin), :
                    ]
                return 0

            lax.fori_loop(0, cwu.shape[0], step, 0)

    for level in (2, 1, 0):
        slack = HALOS[level] - ROWS[level]
        if level == 2:
            correct(2, cwu, cwd, 1, YPAD, 2)
        else:
            x0 = HALOS[level + 1] - HALOS[level] // 2
            correct(level, U[level + 1], D[level + 1], x0, YPAD // 2, slack + 2)
        sweep(level, False, slack + 2)
        update(level, slack + 3)
        sweep(level, False, slack + 3)

    def out_copies(which):
        src, dst = ((U[0], sol_ref), (R[0], res_ref))[which]
        out = []
        for other in range(1, gz_n):
            there = lax.rem(iz + other, gz_n)
            out.append(
                copy(
                    src.at[pl.ds(HALOS[0], nx), there, pl.ds(YPAD, ny), :],
                    dst.at[pl.ds(iz * nx, nx), :, :],
                    o_send.at[which, other],
                    o_recv.at[which, other],
                    (ix, iy, there),
                )
            )
        return out

    def out_local(which):
        src, dst = ((U[0], sol_ref), (R[0], res_ref))[which]

        def step(i, _):
            dst[iz * nx + i] = src[HALOS[0] + i, iz, pl.ds(YPAD, ny), :]
            return 0

        lax.fori_loop(0, nx, step, 0)

    for c in out_copies(0):
        c.start()
    update(0, ROWS[0])
    for c in out_copies(1):
        c.start()
    out_local(0)
    out_local(1)
    for drain in drains:
        drain()
    for which in (0, 1):
        for c in out_copies(which):
            c.wait()


def zero_rows(ref, i, at, value):
    ref[i, :, pl.ds(at, YPAD), :] = value
    return 0


def fits(mesh, shape, inverse_shape):
    gx_n, gy_n, gz_n = (mesh.shape[a] for a in ("gx", "gy", "gz"))
    nx, ny = shape[0] // (gx_n * gz_n), shape[1] // gy_n
    return (
        inverse_shape[0] == LEVELS == 5
        and SWEEPS == 2
        and inverse_shape[2] == 128
        and nx % 8 == 0
        and ny % 32 == 0
        and (shape[1] >> 4) % 8 == 0
        and gz_n <= 2
    )


def fused_body(mesh, right_side, z_faces, xy_coupling, block_inverse):
    gx_n, gy_n, gz_n = (mesh.shape[a] for a in ("gx", "gy", "gz"))
    levels, _, depth = block_inverse.shape
    nx, ny = right_side.shape[0] // gz_n, right_side.shape[1]
    windows = []
    for level in range(levels):
        if level < 3:
            size = ((nx >> level) + 2 * HALOS[level], (ny >> level) + 2 * YPAD)
        else:
            size = ((nx * gx_n * gz_n) >> level, (ny * gy_n) >> level)
        windows.append((size[0], gz_n, size[1], depth))
    vmem = lambda shape: pltpu.VMEM(shape, jnp.float32)
    full3, full4 = windows[3], windows[4]
    pad3 = HALOS[2] // 2 + 1
    c4 = (full4[0] + 2, gz_n, full4[2] + 2 * YPAD, depth)
    c3 = (full3[0] + 2 * pad3, gz_n, full3[2] + 2 * YPAD, depth)
    cw = (windows[2][0] // 2 + 2, gz_n, (ny >> 3) + 20, depth)
    reach = 2 * max(-(-HALOS[k] // (nx >> k)) for k in range(3)) + 1
    slots = 3 * max(reach, 3 * gz_n + 1)
    dma = pltpu.SemaphoreType.DMA
    own = lambda k: (nx >> k, gz_n, ny >> k, depth)
    scratch = (
        [
            pltpu.VMEM((levels, gz_n * depth, gz_n * depth), jnp.bfloat16),
            vmem((levels, gz_n, depth, depth)),
            vmem((gz_n, 1, depth)),
            vmem((gx_n * gz_n, gy_n) + own(3)),
        ]
        + [vmem(w) for w in windows]
        + [vmem(w) for w in windows]
        + [vmem((w[0] + 2,) + w[1:]) for w in windows]
        + [vmem(w) for w in windows]
        + [vmem(w) for w in windows]
        + [vmem(own(1)), vmem(own(2)), vmem(own(3))]
        + [vmem(c4), vmem(c4), vmem(c3), vmem(c3), vmem(cw), vmem(cw)]
        + [dma((gz_n, levels + 1))] * 2
        + [dma((3, slots)), dma((3, slots, gz_n))]
        + [dma((2, max(gx_n * gz_n, gy_n)))] * 2
        + [dma((2, gz_n))] * 2
    )
    in_vmem = pl.BlockSpec(memory_space=pltpu.VMEM)
    return tuple(
        pl.pallas_call(
            functools.partial(cycle_kernel, (gx_n, gy_n, gz_n, nx, ny, depth, levels)),
            out_shape=[jax.ShapeDtypeStruct(right_side.shape, jnp.float32)] * 2,
            in_specs=[
                in_vmem,
                in_vmem,
                pl.BlockSpec(memory_space=pltpu.SMEM),
                in_vmem,
            ],
            out_specs=[in_vmem, in_vmem],
            scratch_shapes=scratch,
            compiler_params=pltpu.CompilerParams(
                collective_id=0, has_side_effects=True, vmem_limit_bytes=60 * 1024 * 1024
            ),
        )(right_side, z_faces.reshape(1, -1), xy_coupling, block_inverse)
    )


def solution(mesh):
    def call(right_side, z_faces, xy_coupling, block_inverse):
        local = body
        if fits(mesh, right_side.shape, block_inverse.shape):
            local = functools.partial(fused_body, mesh)
        return jax.shard_map(
            local,
            mesh=mesh,
            in_specs=(P("gx", "gy", "gz"), P("gz"), P(), P(None, "gz", None)),
            out_specs=(P("gx", "gy", "gz"), P("gx", "gy", "gz")),
            check_vma=False,
        )(right_side, z_faces, xy_coupling, block_inverse)

    return call
```
